32 devices in a mesh: node: 8 (over z, core), expert: 4 (over y, x).
Axes of the slice: x: 2, y: 2, z: 4, core: 2. Of those that a mesh axis runs over, the one named last changes fastest.
Arguments:
- numerators: bfloat16 [8, 4, 1536, 1536], P('node', 'expert'), may hold values from -6 to 6
- push_weights: float32 [8], replicated, may hold values from 0.5 to 2
- tokens: bfloat16 [8, 512, 1536], P('node', 'expert'), may hold values from -6 to 6
- cotangent: bfloat16 [8, 512, 1536], P('node', 'expert'), may hold values from -6 to 6
- routing: int32 [8, 512, 2], P('node', 'expert'), may hold values from 0 to 3, all different within a row; in each aligned block of 128 rows (0 to 127, 128 to 255, ..., all dimensions but the last counted through in order) at most 81 rows name the same one
- gates: float32 [8, 512, 2], P('node', 'expert'), may hold values from 0.1 to 1
Outputs:
- averaged: float32 [4, 1536, 1536], P('expert', 'node')
The draws below stay inside these ranges and needn't reach their ends.
Inputs may be any that keep to these rules, and one draw needn't show every extreme that they name: `routing`: each row names 2 different experts; in each aligned block of 128 rows (the rows of one device) no expert is named by more than 81 rows, and in some block some expert is named by exactly 81 rows.
All inputs are finite; a program needn't handle non-finite values.
Results may differ from the reference program's by a relative error of at most 0.007.
The reference program's roundings to bfloat16 on the way count: a program that leaves them out, or rounds other values in their place, can miss the bound.
Values may be sent and summed in bfloat16 or wider, within the bound.
A program may use at most 64 MiB of HBM per device.

```python
import math
import jax
import jax.numpy as jnp
import numpy as np
from jax import lax

D = 1536
HID = 512
TOP = 2
ROUNDS = 2
TOK_DEV = 128
EXPERTS = 4
NODES = 8
TOK_NODE = 512
CAP = 81
N_EXPERT = 4


def strengthened(values, rng, source, target, parts, factor):
    owner, partner = [(jnp.arange(values.shape[axis_at]) // (values.shape[axis_at] // parts)).reshape([-1 if axis == axis_at else 1 for axis in range(values.ndim)]) for axis_at in (source, target)]
    chosen = jax.random.permutation(rng, parts)[partner]
    strong = (owner == chosen) | (owner == (partner + parts // 2) % parts)
    return jnp.where(strong, factor * values, values)


def shard_levels(rng, shape, shards, least, high):
    gain = 1.0
    for axis_at, shards_of in shards:
        steps = jax.random.uniform(jax.random.fold_in(jax.random.fold_in(rng, 6), axis_at), (shards_of,), jnp.float32, least / len(shards), high / len(shards))
        gain = gain * jnp.repeat(jnp.exp(steps), shape[axis_at] // shards_of).reshape((-1,) + (1,) * (len(shape) - 1 - axis_at))
    return gain


def assign_block(key, own, number, rows, number_of, top, bound, lean):
    ranking = jax.random.permutation(key, number_of)
    crowded, ordinary = portions_of(number_of, rows * top, bound, lean, True), portions_of(number_of, rows * top, bound, lean, False)
    places = jnp.arange(number_of)

    def named(lengths, rotation):
        used = int((lengths > 0).sum())
        fixed = max(1, used // 4)
        moved = fixed + (places - fixed + rotation * (used - fixed)) % max(1, number_of - fixed)
        return jnp.zeros((number_of,), jnp.int32).at[ranking[jnp.where(places < fixed, places, moved)]].set(jnp.asarray(lengths, jnp.int32))

    lengths = jnp.where(number % 4 == 0, named(crowded, number // 4), named(ordinary, number - number // 4 - 1))
    mixed = jax.random.permutation(jax.random.fold_in(own, 3), number_of)
    donor, taker = mixed[0:number_of // 2 * 2:2], mixed[1:number_of // 2 * 2:2]
    room = jnp.minimum(lengths[donor] - 1, bound - lengths[taker]) // 2
    room = jnp.where((donor == ranking[0]) | (taker == ranking[0]) | (lengths[taker] == 0), 0, jnp.maximum(room, 0))
    moved = jax.random.randint(jax.random.fold_in(own, 4), (number_of // 2,), 0, 1 << 20) % (room + 1)
    lengths = lengths.at[donor].add(-moved).at[taker].add(moved)
    items = jnp.searchsorted(jnp.cumsum(lengths), jnp.arange(rows * top), side="right").astype(jnp.int32)
    table = items.reshape(top, rows).T
    table = table[jax.random.permutation(jax.random.fold_in(own, 1), rows)]
    rotation = jax.random.randint(jax.random.fold_in(own, 2), (rows, 1), 0, top)
    return jnp.take_along_axis(table, (jnp.arange(top)[None, :] + rotation) % top, axis=1)


def portions_of(number_of, total, bound, lean, full):
    weights = [(1 << 20) // math.isqrt(grade ** lean) + 1 for grade in range(1, number_of + 1)]
    largest = bound if full else min(bound, max(-(-total // number_of), total * weights[0] // sum(weights)))
    least = 1 if total - largest >= number_of - 1 else 0
    given, rest = [largest] + [least] * (number_of - 1), total - largest - least * (number_of - 1)
    while rest > 0:
        free = [i for i in range(1, number_of) if given[i] < largest] or [i for i in range(1, number_of) if given[i] < bound]
        mass, remaining = sum([weights[i] for i in free]), rest
        for i in free:
            extra = min(bound - given[i], max(1, remaining * weights[i] // mass), rest)
            given[i] = given[i] + extra
            rest = rest - extra
    return np.array(given)


def bell_draw(stream_key, shape, spread, bound, split=(), dtype=jnp.bfloat16):
    values = jax.random.normal(stream_key, shape, jnp.float32) * spread
    if len(split) > 0:
        values = shard_levels(stream_key, shape, split, -0.22, 0.18) * values
    return jnp.clip(values, min=-bound, max=bound).astype(dtype)


def bell_draw_with(key, extent, deviation, reach, split, heavy, dtype=jnp.bfloat16):
    array = deviation * jax.random.normal(key, extent, jnp.float32)
    if split:
        array = array * shard_levels(key, extent, split, -0.22, 0.18)
    return jnp.clip(strengthened(array, jax.random.fold_in(key, 3), *heavy), -reach, reach).astype(dtype)


def setup_inputs(seed: int = 0) -> dict:
    keys = jax.random.split(jax.random.key(seed), 7)
    numerators = bell_draw_with(keys[0], (NODES, EXPERTS, D, 3 * HID), 1.0, 6.0, ((0, 8), (1, 4)), (0, 2, 8, 2.0))
    push_weights = jnp.clip(jnp.exp(jax.random.uniform(keys[1], (NODES,), jnp.float32, math.log(0.5), math.log(2.0))), 0.5, 2.0)
    tokens = bell_draw(keys[2], (NODES, TOK_NODE, D), 1.0, 6.0, ((0, 8), (1, 4)))
    cotangent = bell_draw(keys[3], (NODES, TOK_NODE, D), 1.0, 6.0, ((0, 8), (1, 4)))
    routing_keys = jax.random.split(jax.random.fold_in(keys[4], 1), NODES * TOK_NODE // TOK_DEV)
    routing_turns = jax.random.permutation(jax.random.fold_in(keys[4], 3), NODES * TOK_NODE // TOK_DEV)
    routing = jax.vmap(lambda own, number: assign_block(jax.random.fold_in(keys[4], 2), own, number, TOK_DEV, EXPERTS, TOP, CAP, 1))(routing_keys, routing_turns).reshape((NODES, TOK_NODE, TOP))
    gates = jnp.clip(jnp.exp(math.log(1.0) - 2.3025851 * jax.random.uniform(keys[5], (NODES, TOK_NODE, TOP), jnp.float32) ** shard_levels(keys[5], (NODES, TOK_NODE, TOP), ((0, 8), (1, 4)), -0.2, 0.2)), 0.1, 1.0)
    return dict(numerators=numerators, push_weights=push_weights, tokens=tokens, cotangent=cotangent, routing=routing, gates=gates)


step_size = 1.0

def expert_update(weights, buffer_inputs, buffer_gradients):
    hidden_units = weights.shape[1] // 3
    model_scale = 1.0 / math.sqrt(weights.shape[0])
    hidden_scale = 1.0 / math.sqrt(hidden_units)
    gate_weight_matrix = weights[:, :hidden_units]
    upward_weight = weights[:, hidden_units:2 * hidden_units]
    downward_weight = weights[:, 2 * hidden_units:]
    gate_pre = jnp.dot(buffer_inputs, gate_weight_matrix, preferred_element_type=jnp.float32) * model_scale
    upper_pre = jnp.dot(buffer_inputs, upward_weight, preferred_element_type=jnp.float32) * model_scale
    sigmoid_gate = jax.nn.sigmoid(gate_pre)
    gated_hidden = (gate_pre * sigmoid_gate * upper_pre).astype(jnp.bfloat16)
    grad_down = jnp.dot(buffer_gradients.T, gated_hidden, preferred_element_type=jnp.float32) * hidden_scale
    grad_act = jnp.dot(buffer_gradients, downward_weight, preferred_element_type=jnp.float32) * hidden_scale
    gate_gradient = (grad_act * upper_pre * sigmoid_gate * (1.0 + gate_pre * (1.0 - sigmoid_gate))).astype(jnp.bfloat16)
    upward_gradient = (grad_act * gate_pre * sigmoid_gate).astype(jnp.bfloat16)
    grad_wgate = jnp.dot(buffer_inputs.T, gate_gradient, preferred_element_type=jnp.float32) * model_scale
    grad_wupper = jnp.dot(buffer_inputs.T, upward_gradient, preferred_element_type=jnp.float32) * model_scale
    return jnp.concatenate([grad_wgate, grad_wupper, grad_down], axis=1)

def node_step(current, weight, node_tokens, node_cot, node_routes, node_gates):
    params = (current.astype(jnp.float32) / weight).astype(jnp.bfloat16)
    slot_rows = CAP * N_EXPERT
    updates = []
    for expert in range(EXPERTS):
        chosen = node_routes == expert
        present = jnp.any(chosen, axis=1)
        gate_sum = lax.optimization_barrier(jnp.sum(jnp.where(chosen, node_gates, 0.0), axis=1))
        ordering = jnp.argsort(jnp.where(present, 0, 1).astype(jnp.int32), stable=True)[:slot_rows]
        occupied = present[ordering]
        buffer_inputs = jnp.where(occupied[:, None], node_tokens[ordering], 0.0).astype(jnp.bfloat16)
        scaled = gate_sum[ordering][:, None] * node_cot[ordering].astype(jnp.float32)
        buffer_gradients = jnp.where(occupied[:, None], scaled, 0.0).astype(jnp.bfloat16)
        gradients = expert_update(params[expert], buffer_inputs, buffer_gradients)
        updates.append((current[expert].astype(jnp.float32) - step_size * gradients).astype(jnp.bfloat16))
    return jnp.stack(updates)

def reference(numerators, push_weights, tokens, cotangent, routing, gates):
    current = numerators
    weights_now = push_weights
    result = jnp.zeros(numerators.shape[1:], jnp.float32)
    for round_index in range(ROUNDS):
        offset = 2 ** round_index

        def one_node(packed):
            return node_step(packed[0], packed[1], packed[2], packed[3], packed[4], packed[5])
        pushed = lax.map(one_node, (current, weights_now, tokens, cotangent, routing, gates))
        mixed_weights = (weights_now + jnp.roll(weights_now, offset)) / 2.0
        rolled = jnp.roll(pushed, offset, axis=0)
        if round_index < ROUNDS - 1:
            current = ((pushed.astype(jnp.float32) + rolled.astype(jnp.float32)) / 2.0).astype(jnp.bfloat16)
            weights_now = mixed_weights
        else:

            def accumulate(carry, packed):
                first, second, weight = packed
                mixed = (first.astype(jnp.float32) + second.astype(jnp.float32)) / 2.0
                return (carry + mixed / weight / NODES, None)
            result, unused = lax.scan(accumulate, result, (pushed, rolled, mixed_weights))
    return result
```

```python
import math

import jax
import jax.numpy as jnp
from jax import lax
from jax.sharding import PartitionSpec as P

ROUNDS = 2
step_size = 1.0


def passed_along(shard, axis, by):
    count = lax.axis_size(axis)
    return lax.ppermute(shard, axis, [(i, (i + by) % count) for i in range(count)])


def swapped(shard, axis, bits):
    count = lax.axis_size(axis)
    return lax.ppermute(shard, axis, [(i, i ^ bits) for i in range(count)])


def gathered(own, gate_rows):
    count = lax.axis_size("expert")
    me = lax.axis_index("expert")
    if count != 4:
        return (
            lax.all_gather(own, "expert", axis=0, tiled=True),
            gate_rows.reshape(-1),
        )
    half = own.shape[0] // 2
    by_x = swapped(own, "expert", 1)
    by_y = swapped(own, "expert", 2)
    far_top = swapped(by_x[:half], "expert", 2)
    far_bottom = swapped(by_y[half:], "expert", 1)
    order = [lax.dynamic_index_in_dim(gate_rows, me ^ k, keepdims=False) for k in range(4)]
    return (
        jnp.concatenate([own, by_x, by_y, far_top, far_bottom], axis=0),
        jnp.concatenate(order),
    )


def reduced(pushed, factor):
    count = lax.axis_size("node")
    node = lax.axis_index("node")
    chips = count // 2
    chip, core = node // 2, node % 2
    blocks = pushed.reshape(chips, 2, pushed.shape[0] // count, pushed.shape[1])
    away = lax.dynamic_index_in_dim(blocks, 1 - core, axis=1, keepdims=False)
    own = lax.dynamic_index_in_dim(blocks, core, axis=1, keepdims=False)
    came = swapped(away, "node", 1)
    own_factor = lax.dynamic_index_in_dim(factor, node, keepdims=False)
    other_factor = lax.dynamic_index_in_dim(factor, node ^ 1, keepdims=False)

    def term(at):
        at = jnp.clip(at, 0, chips - 1)
        mine = lax.dynamic_index_in_dim(own, at, keepdims=False).astype(jnp.float32)
        theirs = lax.dynamic_index_in_dim(came, at, keepdims=False).astype(jnp.float32)
        return mine * own_factor + theirs * other_factor

    up = down = None
    for step in range(1, chips):
        rising = term(chips - step + chip)
        falling = term(chip + step - chips)
        if up is not None:
            rising, falling = rising + up.astype(jnp.float32), falling + down.astype(jnp.float32)
        up_pairs = [
            (2 * c + k, 2 * c + 2 + k) for c in range(min(step, chips - 1)) for k in range(2)
        ]
        down_pairs = [
            (2 * c + k, 2 * c - 2 + k) for c in range(max(chips - step, 1), chips) for k in range(2)
        ]
        up = lax.ppermute(rising.astype(jnp.bfloat16), "node", up_pairs)
        down = lax.ppermute(falling.astype(jnp.bfloat16), "node", down_pairs)
    total = term(chip)
    if up is not None:
        total = total + up.astype(jnp.float32) + down.astype(jnp.float32)
    return total


def local(numerators, push_weights, tokens, cotangent, routing, gates):
    node_count = lax.axis_size("node")
    node = lax.axis_index("node")
    expert_count = numerators.shape[1] * lax.axis_size("expert")
    model_dim = tokens.shape[2]
    chosen = routing[0][:, :, None] == jnp.arange(expert_count, dtype=jnp.int32)
    dense = jnp.sum(jnp.where(chosen, gates[0][:, :, None], 0.0), axis=1).T
    gate_rows = lax.all_to_all(dense, "expert", split_axis=0, concat_axis=0, tiled=True)
    own = jnp.concatenate([tokens[0], cotangent[0]], axis=1)
    rows, row_gates = gathered(own, gate_rows)
    inputs = rows[:, :model_dim]
    gradients = (rows[:, model_dim:].astype(jnp.float32) * row_gates[:, None]).astype(jnp.bfloat16)
    current = numerators[0, 0]
    hidden = current.shape[1] // 3
    cuts = 4
    part = hidden // cuts
    slices = [
        jnp.concatenate(
            [current[:, j * hidden + k * part : j * hidden + (k + 1) * part] for j in range(3)],
            axis=1,
        )
        for k in range(cuts)
    ]
    weights_now = push_weights
    mixed_weights = push_weights
    offset = 1
    for round_index in range(ROUNDS):
        offset = 2**round_index
        own_weight = lax.dynamic_index_in_dim(weights_now, node, keepdims=False)
        pushed = []
        for z in slices:
            params = (z.astype(jnp.float32) / own_weight).astype(jnp.bfloat16)
            grads = slice_grads(params, inputs, gradients, hidden)
            pushed.append((z.astype(jnp.float32) - step_size * grads).astype(jnp.bfloat16))
        mixed_weights = (weights_now + jnp.roll(weights_now, offset)) / 2.0
        if round_index < ROUNDS - 1:
            slices = [
                (
                    (p.astype(jnp.float32) + passed_along(p, "node", offset).astype(jnp.float32))
                    / 2.0
                ).astype(jnp.bfloat16)
                for p in pushed
            ]
            weights_now = mixed_weights
    factor = (0.5 / mixed_weights + 0.5 / jnp.roll(mixed_weights, -offset)) / node_count
    outs = [reduced(p, factor) for p in pushed]
    whole = jnp.concatenate(
        [outs[k][:, j * part : (j + 1) * part] for j in range(3) for k in range(cuts)], axis=1
    )
    return whole[None]


def slice_grads(weights, inputs, gradients, hidden):
    part = weights.shape[1] // 3
    model_scale = 1.0 / math.sqrt(weights.shape[0])
    hidden_scale = 1.0 / math.sqrt(hidden)
    f32 = jnp.float32

    def forward(a, b):
        return lax.dot_general(a, b, (((1,), (0,)), ((), ())), preferred_element_type=f32)

    def outer(a, b):
        return lax.dot_general(a, b, (((0,), (0,)), ((), ())), preferred_element_type=f32)

    pre = forward(inputs, weights[:, : 2 * part]) * model_scale
    gate_pre, upper_pre = pre[:, :part], pre[:, part:]
    sigmoid_gate = jax.nn.sigmoid(gate_pre)
    gated_hidden = (gate_pre * sigmoid_gate * upper_pre).astype(jnp.bfloat16)
    grad_act = forward(gradients, weights[:, 2 * part :]) * hidden_scale
    gate_gradient = (
        grad_act * upper_pre * sigmoid_gate * (1.0 + gate_pre * (1.0 - sigmoid_gate))
    ).astype(jnp.bfloat16)
    upward_gradient = (grad_act * gate_pre * sigmoid_gate).astype(jnp.bfloat16)
    both = jnp.concatenate([gate_gradient, upward_gradient], axis=1)
    return jnp.concatenate(
        [outer(inputs, both) * model_scale, outer(gradients, gated_hidden) * hidden_scale], axis=1
    )


def solution(mesh):
    placed = (
        P("node", "expert", None, None),
        P(),
        P("node", "expert", None),
        P("node", "expert", None),
        P("node", "expert", None),
        P("node", "expert", None),
    )
    return jax.shard_map(
        local, mesh=mesh, in_specs=placed, out_specs=P("expert", "node", None), check_vma=False
    )
```

```python
import functools
import math

import jax
import jax.numpy as jnp
from jax import lax
from jax.experimental import pallas as pl
from jax.experimental.pallas import tpu as pltpu
from jax.sharding import PartitionSpec as P

step_size = 1.0


def swapped(shard, axis, bits):
    count = lax.axis_size(axis)
    return lax.ppermute(shard, axis, [(i, i ^ bits) for i in range(count)])


def gathered(own, gate_rows):
    count = lax.axis_size("expert")
    me = lax.axis_index("expert")
    if count != 4:
        return (
            lax.all_gather(own, "expert", axis=0, tiled=True),
            gate_rows.reshape(-1),
        )
    half = own.shape[0] // 2
    by_x = swapped(own, "expert", 1)
    by_y = swapped(own, "expert", 2)
    far_top = swapped(by_x[:half], "expert", 2)
    far_bottom = swapped(by_y[half:], "expert", 1)
    order = [lax.dynamic_index_in_dim(gate_rows, me ^ k, keepdims=False) for k in range(4)]
    return (
        jnp.concatenate([own, by_x, by_y, far_top, far_bottom], axis=0),
        jnp.concatenate(order),
    )


def steps_kernel(
    count, cuts, scal, z_ref, x_ref, g_ref, xt_ref, gt_ref, out_ref,
    zc, par, hid, first, arrived, second, came, sent, got,
    ex_send, ex_recv, pair_send, pair_recv, line_send, line_recv,
):
    bf16, f32 = jnp.bfloat16, jnp.float32
    node = lax.axis_index("node")
    chips = count // 2
    chip, core = node // 2, node % 2
    other = chip * 2 + (1 - core)
    depth, width = zc.shape
    part = width // 3
    hidden = part * cuts
    tokens = x_ref.shape[0]
    model_scale = 1.0 / math.sqrt(depth)
    hidden_scale = 1.0 / math.sqrt(hidden)
    rows = depth // count
    tile_d, tile_t = math.gcd(depth, 256), math.gcd(tokens, 128)

    barrier = pltpu.get_barrier_semaphore()
    for by in (1, count - 1, 2, count - 2):
        pl.semaphore_signal(
            barrier, inc=1, device_id={"node": (node + by) % count},
            device_id_type=pl.DeviceIdType.MESH,
        )
    pl.semaphore_wait(barrier, 4)

    def remote(src, dst, send, recv, to):
        return pltpu.make_async_remote_copy(
            src_ref=src, dst_ref=dst, send_sem=send, recv_sem=recv,
            device_id={"node": to}, device_id_type=pl.DeviceIdType.MESH,
        )

    def exchange(k):
        return remote(
            first.at[k], arrived.at[k], ex_send.at[k], ex_recv.at[k], (node + 1) % count
        )

    def pair(k):
        return remote(
            second.at[k, :, 1 - core], came.at[k], pair_send.at[k], pair_recv.at[k], other
        )

    def line(way, k, t):
        to = (node + (2 if way == 0 else count - 2)) % count
        return remote(
            sent.at[way, k, t], got.at[way, k, t], line_send.at[way, k, t],
            line_recv.at[way, k, t], to,
        )

    def hidden_gradients():
        @pl.loop(0, tokens // tile_t)
        def _(i):
            at = pl.ds(pl.multiple_of(i * tile_t, tile_t), tile_t)
            pre = jnp.dot(x_ref[at, :], par[:, : 2 * part], preferred_element_type=f32)
            act = jnp.dot(g_ref[at, :], par[:, 2 * part :], preferred_element_type=f32)
            gate = pre[:, :part] * model_scale
            upper = pre[:, part:] * model_scale
            act = act * hidden_scale
            sig = jax.nn.sigmoid(gate)
            hid[at, :part] = (act * upper * sig * (1.0 + gate * (1.0 - sig))).astype(bf16)
            hid[at, part : 2 * part] = (act * gate * sig).astype(bf16)
            hid[at, 2 * part :] = (gate * sig * upper).astype(bf16)

    def moved(at):
        both = jnp.dot(xt_ref[at, :], hid[:, : 2 * part], preferred_element_type=f32)
        down = jnp.dot(gt_ref[at, :], hid[:, 2 * part :], preferred_element_type=f32)
        grads = jnp.concatenate([both * model_scale, down * hidden_scale], axis=1)
        return (zc[at, :].astype(f32) - step_size * grads).astype(bf16)

    def round_one(k, carry):
        weight = scal[0]

        @pl.loop(0, depth // tile_d)
        def _(i):
            at = pl.ds(pl.multiple_of(i * tile_d, tile_d), tile_d)
            for j in range(3):
                to = pl.ds(pl.multiple_of(j * hidden + k * part, part), part)
                z = z_ref[at, to]
                zc[at, j * part : (j + 1) * part] = z
                par[at, j * part : (j + 1) * part] = (z.astype(f32) / weight).astype(bf16)

        def outer(i):
            at = pl.ds(pl.multiple_of(i * tile_d, tile_d), tile_d)
            first[k, at, :] = moved(at)

        hidden_gradients()
        pl.loop(0, depth // tile_d)(outer)
        exchange(k).start()
        return carry

    def round_two(k):
        weight = scal[1]
        exchange(k).wait_recv()

        @pl.loop(0, depth // tile_d)
        def _(i):
            at = pl.ds(pl.multiple_of(i * tile_d, tile_d), tile_d)
            z = ((first[k, at, :].astype(f32) + arrived[k, at, :].astype(f32)) / 2.0).astype(bf16)
            zc[at, :] = z
            par[at, :] = (z.astype(f32) / weight).astype(bf16)

        def outer(i):
            value = moved(pl.ds(pl.multiple_of(i * 2 * rows, 2 * rows), 2 * rows))
            second[k, i, 0] = value[:rows]
            second[k, i, 1] = value[rows:]

        hidden_gradients()
        pl.loop(0, chips)(outer)
        pair(k).start()

    def term(k, t):
        return second[k, t, core].astype(f32) * scal[2] + came[k, t].astype(f32) * scal[3]

    def send_sums(k):
        pair(k).wait_recv()

        def rising(j, carry):
            t = chips - 1 - j
            sent[0, k, t] = term(k, t).astype(bf16)

            @pl.when(chip > 0)
            def _():
                line(0, k, t).wait_recv()
                sent[0, k, t] = (term(k, t) + got[0, k, t].astype(f32)).astype(bf16)

            line(0, k, t).start()
            return carry

        def falling(t, carry):
            sent[1, k, t] = term(k, t).astype(bf16)

            @pl.when(chip < chips - 1)
            def _():
                line(1, k, t).wait_recv()
                sent[1, k, t] = (term(k, t) + got[1, k, t].astype(f32)).astype(bf16)

            line(1, k, t).start()
            return carry

        @pl.when(chip * 2 < chips)
        def _():
            lax.fori_loop(0, chips - 1 - chip, rising, 0)
            lax.fori_loop(0, chip, falling, 0)

        @pl.when(chip * 2 >= chips)
        def _():
            lax.fori_loop(0, chip, falling, 0)
            lax.fori_loop(0, chips - 1 - chip, rising, 0)

    lax.fori_loop(0, cuts, round_one, 0)

    def second_phase(k, carry):
        round_two(k)

        @pl.when(k > 0)
        def _():
            send_sums(k - 1)

        return carry

    lax.fori_loop(0, cuts, second_phase, 0)
    send_sums(cuts - 1)

    def finish(k, j, value):
        out_ref[:, j * hidden + k * part : j * hidden + (k + 1) * part] = value

    for k in range(cuts):
        for j in range(3):
            cols = slice(j * part, (j + 1) * part)
            finish(
                k, j,
                second[k, chip, core, :, cols].astype(f32) * scal[2]
                + came[k, chip, :, cols].astype(f32) * scal[3],
            )
        for way, there in ((0, chip > 0), (1, chip < chips - 1)):

            @pl.when(there)
            def _():
                line(way, k, chip).wait_recv()
                for j in range(3):
                    at = slice(j * hidden + k * part, j * hidden + (k + 1) * part)
                    cols = slice(j * part, (j + 1) * part)
                    out_ref[:, at] = out_ref[:, at] + got[way, k, chip, :, cols].astype(f32)

    def drain(k, carry):
        exchange(k).wait_send()
        pair(k).wait_send()

        def up(t, c):
            line(0, k, t).wait_send()
            return c

        def down(t, c):
            line(1, k, t).wait_send()
            return c

        lax.fori_loop(chip + 1, chips, up, 0)
        lax.fori_loop(0, chip, down, 0)
        return carry

    lax.fori_loop(0, cuts, drain, 0)


def both_rounds(scalars, z, inputs, gradients, count):
    bf16 = jnp.bfloat16
    depth, columns = z.shape
    hidden = columns // 3
    part = math.gcd(hidden, 128)
    cuts = hidden // part
    width = 3 * part
    chips, rows = count // 2, depth // count
    vmem = pl.BlockSpec(memory_space=pltpu.VMEM)
    dma = pltpu.SemaphoreType.DMA
    return pl.pallas_call(
        functools.partial(steps_kernel, count, cuts),
        out_shape=jax.ShapeDtypeStruct((rows, columns), jnp.float32),
        in_specs=[pl.BlockSpec(memory_space=pltpu.SMEM)] + [vmem] * 5,
        out_specs=vmem,
        scratch_shapes=[
            pltpu.VMEM((depth, width), bf16),
            pltpu.VMEM((depth, width), bf16),
            pltpu.VMEM((inputs.shape[0], width), bf16),
            pltpu.VMEM((cuts, depth, width), bf16),
            pltpu.VMEM((cuts, depth, width), bf16),
            pltpu.VMEM((cuts, chips, 2, rows, width), bf16),
            pltpu.VMEM((cuts, chips, rows, width), bf16),
            pltpu.VMEM((2, cuts, chips, rows, width), bf16),
            pltpu.VMEM((2, cuts, chips, rows, width), bf16),
            dma((cuts,)),
            dma((cuts,)),
            dma((cuts,)),
            dma((cuts,)),
            dma((2, cuts, chips)),
            dma((2, cuts, chips)),
        ],
        compiler_params=pltpu.CompilerParams(
            collective_id=0, has_side_effects=True, vmem_limit_bytes=60 * 1024 * 1024
        ),
    )(scalars, z, inputs, gradients, inputs.T, gradients.T)


def local(numerators, push_weights, tokens, cotangent, routing, gates):
    node_count = lax.axis_size("node")
    node = lax.axis_index("node")
    expert_count = numerators.shape[1] * lax.axis_size("expert")
    model_dim = tokens.shape[2]
    chosen = routing[0][:, :, None] == jnp.arange(expert_count, dtype=jnp.int32)
    dense = jnp.sum(jnp.where(chosen, gates[0][:, :, None], 0.0), axis=1).T
    gate_rows = lax.all_to_all(dense, "expert", split_axis=0, concat_axis=0, tiled=True)
    own = jnp.concatenate([tokens[0], cotangent[0]], axis=1)
    rows, row_gates = gathered(own, gate_rows)
    inputs = rows[:, :model_dim]
    gradients = (rows[:, model_dim:].astype(jnp.float32) * row_gates[:, None]).astype(jnp.bfloat16)
    later_weights = (push_weights + jnp.roll(push_weights, 1)) / 2.0
    last_weights = (later_weights + jnp.roll(later_weights, 2)) / 2.0
    factor = (0.5 / last_weights + 0.5 / jnp.roll(last_weights, -2)) / node_count

    def at(values, index):
        return lax.dynamic_index_in_dim(values, index, keepdims=False)

    scalars = jnp.stack(
        [at(push_weights, node), at(later_weights, node), at(factor, node), at(factor, node ^ 1)]
    )
    return both_rounds(scalars, numerators[0, 0], inputs, gradients, node_count)[None]


def solution(mesh):
    placed = (
        P("node", "expert", None, None),
        P(),
        P("node", "expert", None),
        P("node", "expert", None),
        P("node", "expert", None),
        P("node", "expert", None),
    )
    return jax.shard_map(
        local, mesh=mesh, in_specs=placed, out_specs=P("expert", "node", None), check_vma=False
    )
```

```python
import functools
import math

import jax
import jax.numpy as jnp
from jax import lax
from jax.experimental import pallas as pl
from jax.experimental.pallas import tpu as pltpu
from jax.sharding import PartitionSpec as P

step_size = 1.0


def swapped(shard, axis, bits):
    count = lax.axis_size(axis)
    return lax.ppermute(shard, axis, [(i, i ^ bits) for i in range(count)])


def gathered(own, gate_rows):
    count = lax.axis_size("expert")
    me = lax.axis_index("expert")
    if count != 4:
        return (
            lax.all_gather(own, "expert", axis=0, tiled=True),
            gate_rows.reshape(-1),
        )
    half = own.shape[0] // 2
    by_x = swapped(own, "expert", 1)
    by_y = swapped(own, "expert", 2)
    far_top = swapped(by_x[:half], "expert", 2)
    far_bottom = swapped(by_y[half:], "expert", 1)
    order = [lax.dynamic_index_in_dim(gate_rows, me ^ k, keepdims=False) for k in range(4)]
    return (
        jnp.concatenate([own, by_x, by_y, far_top, far_bottom], axis=0),
        jnp.concatenate(order),
    )


def steps_kernel(
    count, cuts, scal, z_ref, x_ref, g_ref, out_ref,
    xt_ref, gt_ref, zc, par, hid, first, arrived, second, came, sent, got,
    ex_send, ex_recv, pair_send, pair_recv, line_send, line_recv,
):
    bf16, f32 = jnp.bfloat16, jnp.float32
    node = lax.axis_index("node")
    chips = count // 2
    chip, core = node // 2, node % 2
    other = chip * 2 + (1 - core)
    depth, width = zc.shape
    part = width // 3
    hidden = part * cuts
    tokens = x_ref.shape[0]
    model_scale = 1.0 / math.sqrt(depth)
    hidden_scale = 1.0 / math.sqrt(hidden)
    rows = depth // count
    tile_d, tile_t = math.gcd(depth, 256), math.gcd(tokens, 128)

    barrier = pltpu.get_barrier_semaphore()
    for by in (1, count - 1, 2, count - 2):
        pl.semaphore_signal(
            barrier, inc=1, device_id={"node": (node + by) % count},
            device_id_type=pl.DeviceIdType.MESH,
        )
    pl.semaphore_wait(barrier, 4)

    for i in range(tokens // tile_t):
        at = slice(i * tile_t, (i + 1) * tile_t)
        xt_ref[:, at] = x_ref[at, :].T
        gt_ref[:, at] = g_ref[at, :].T

    def remote(src, dst, send, recv, to):
        return pltpu.make_async_remote_copy(
            src_ref=src, dst_ref=dst, send_sem=send, recv_sem=recv,
            device_id={"node": to}, device_id_type=pl.DeviceIdType.MESH,
        )

    def exchange(k):
        return remote(
            first.at[k], arrived.at[k], ex_send.at[k], ex_recv.at[k], (node + 1) % count
        )

    def pair(k):
        return remote(
            second.at[k, :, 1 - core], came.at[k], pair_send.at[k], pair_recv.at[k], other
        )

    def line(way, k, t):
        to = (node + (2 if way == 0 else count - 2)) % count
        return remote(
            sent.at[way, k, t], got.at[way, k, t], line_send.at[way, k, t],
            line_recv.at[way, k, t], to,
        )

    def hidden_gradients():
        @pl.loop(0, tokens // tile_t)
        def _(i):
            at = pl.ds(pl.multiple_of(i * tile_t, tile_t), tile_t)
            pre = jnp.dot(x_ref[at, :], par[:, : 2 * part], preferred_element_type=f32)
            act = jnp.dot(g_ref[at, :], par[:, 2 * part :], preferred_element_type=f32)
            gate = pre[:, :part] * model_scale
            upper = pre[:, part:] * model_scale
            act = act * hidden_scale
            sig = jax.nn.sigmoid(gate)
            hid[at, :part] = (act * upper * sig * (1.0 + gate * (1.0 - sig))).astype(bf16)
            hid[at, part : 2 * part] = (act * gate * sig).astype(bf16)
            hid[at, 2 * part :] = (gate * sig * upper).astype(bf16)

    def moved(at):
        both = jnp.dot(xt_ref[at, :], hid[:, : 2 * part], preferred_element_type=f32)
        down = jnp.dot(gt_ref[at, :], hid[:, 2 * part :], preferred_element_type=f32)
        grads = jnp.concatenate([both * model_scale, down * hidden_scale], axis=1)
        return (zc[at, :].astype(f32) - step_size * grads).astype(bf16)

    def round_one(k, carry):
        weight = scal[0]

        @pl.loop(0, depth // tile_d)
        def _(i):
            at = pl.ds(pl.multiple_of(i * tile_d, tile_d), tile_d)
            for j in range(3):
                to = pl.ds(pl.multiple_of(j * hidden + k * part, part), part)
                z = z_ref[at, to]
                zc[at, j * part : (j + 1) * part] = z
                par[at, j * part : (j + 1) * part] = (z.astype(f32) / weight).astype(bf16)

        def outer(i):
            at = pl.ds(pl.multiple_of(i * tile_d, tile_d), tile_d)
            first[k, at, :] = moved(at)

        hidden_gradients()
        pl.loop(0, depth // tile_d)(outer)
        exchange(k).start()
        return carry

    def round_two(k):
        weight = scal[1]
        exchange(k).wait_recv()

        @pl.loop(0, depth // tile_d)
        def _(i):
            at = pl.ds(pl.multiple_of(i * tile_d, tile_d), tile_d)
            z = ((first[k, at, :].astype(f32) + arrived[k, at, :].astype(f32)) / 2.0).astype(bf16)
            zc[at, :] = z
            par[at, :] = (z.astype(f32) / weight).astype(bf16)

        def outer(i):
            value = moved(pl.ds(pl.multiple_of(i * 2 * rows, 2 * rows), 2 * rows))
            second[k, i, 0] = value[:rows]
            second[k, i, 1] = value[rows:]

        hidden_gradients()
        pl.loop(0, chips)(outer)
        pair(k).start()

    def term(k, t):
        return second[k, t, core].astype(f32) * scal[2] + came[k, t].astype(f32) * scal[3]

    def send_sums(k):
        pair(k).wait_recv()

        def rising(j, carry):
            t = chips - 1 - j
            sent[0, k, t] = term(k, t).astype(bf16)

            @pl.when(chip > 0)
            def _():
                line(0, k, t).wait_recv()
                sent[0, k, t] = (term(k, t) + got[0, k, t].astype(f32)).astype(bf16)

            line(0, k, t).start()
            return carry

        def falling(t, carry):
            sent[1, k, t] = term(k, t).astype(bf16)

            @pl.when(chip < chips - 1)
            def _():
                line(1, k, t).wait_recv()
                sent[1, k, t] = (term(k, t) + got[1, k, t].astype(f32)).astype(bf16)

            line(1, k, t).start()
            return carry

        @pl.when(chip * 2 < chips)
        def _():
            lax.fori_loop(0, chips - 1 - chip, rising, 0)
            lax.fori_loop(0, chip, falling, 0)

        @pl.when(chip * 2 >= chips)
        def _():
            lax.fori_loop(0, chip, falling, 0)
            lax.fori_loop(0, chips - 1 - chip, rising, 0)

    lax.fori_loop(0, cuts, round_one, 0)

    def second_phase(k, carry):
        round_two(k)

        @pl.when(k > 0)
        def _():
            send_sums(k - 1)

        return carry

    lax.fori_loop(0, cuts, second_phase, 0)
    send_sums(cuts - 1)

    def finish(k, j, value):
        out_ref[:, j * hidden + k * part : j * hidden + (k + 1) * part] = value

    for k in range(cuts):
        for j in range(3):
            cols = slice(j * part, (j + 1) * part)
            finish(
                k, j,
                second[k, chip, core, :, cols].astype(f32) * scal[2]
                + came[k, chip, :, cols].astype(f32) * scal[3],
            )
        for way, there in ((0, chip > 0), (1, chip < chips - 1)):

            @pl.when(there)
            def _():
                line(way, k, chip).wait_recv()
                for j in range(3):
                    at = slice(j * hidden + k * part, j * hidden + (k + 1) * part)
                    cols = slice(j * part, (j + 1) * part)
                    out_ref[:, at] = out_ref[:, at] + got[way, k, chip, :, cols].astype(f32)

    def drain(k, carry):
        exchange(k).wait_send()
        pair(k).wait_send()

        def up(t, c):
            line(0, k, t).wait_send()
            return c

        def down(t, c):
            line(1, k, t).wait_send()
            return c

        lax.fori_loop(chip + 1, chips, up, 0)
        lax.fori_loop(0, chip, down, 0)
        return carry

    lax.fori_loop(0, cuts, drain, 0)


def both_rounds(scalars, z, inputs, gradients, count):
    bf16 = jnp.bfloat16
    depth, columns = z.shape
    hidden = columns // 3
    part = math.gcd(hidden, 128)
    cuts = hidden // part
    width = 3 * part
    chips, rows = count // 2, depth // count
    vmem = pl.BlockSpec(memory_space=pltpu.VMEM)
    dma = pltpu.SemaphoreType.DMA
    return pl.pallas_call(
        functools.partial(steps_kernel, count, cuts),
        out_shape=jax.ShapeDtypeStruct((rows, columns), jnp.float32),
        in_specs=[pl.BlockSpec(memory_space=pltpu.SMEM)] + [vmem] * 3,
        out_specs=vmem,
        scratch_shapes=[
            pltpu.VMEM((depth, inputs.shape[0]), bf16),
            pltpu.VMEM((depth, inputs.shape[0]), bf16),
            pltpu.VMEM((depth, width), bf16),
            pltpu.VMEM((depth, width), bf16),
            pltpu.VMEM((inputs.shape[0], width), bf16),
            pltpu.VMEM((cuts, depth, width), bf16),
            pltpu.VMEM((cuts, depth, width), bf16),
            pltpu.VMEM((cuts, chips, 2, rows, width), bf16),
            pltpu.VMEM((cuts, chips, rows, width), bf16),
            pltpu.VMEM((2, cuts, chips, rows, width), bf16),
            pltpu.VMEM((2, cuts, chips, rows, width), bf16),
            dma((cuts,)),
            dma((cuts,)),
            dma((cuts,)),
            dma((cuts,)),
            dma((2, cuts, chips)),
            dma((2, cuts, chips)),
        ],
        compiler_params=pltpu.CompilerParams(
            collective_id=0, has_side_effects=True, vmem_limit_bytes=60 * 1024 * 1024
        ),
    )(scalars, z, inputs, gradients)


def local(numerators, push_weights, tokens, cotangent, routing, gates):
    node_count = lax.axis_size("node")
    node = lax.axis_index("node")
    expert_count = numerators.shape[1] * lax.axis_size("expert")
    model_dim = tokens.shape[2]
    chosen = routing[0][:, :, None] == jnp.arange(expert_count, dtype=jnp.int32)
    dense = jnp.sum(jnp.where(chosen, gates[0][:, :, None], 0.0), axis=1).T
    gate_rows = lax.all_to_all(dense, "expert", split_axis=0, concat_axis=0, tiled=True)
    own = jnp.concatenate([tokens[0], cotangent[0]], axis=1)
    rows, row_gates = gathered(own, gate_rows)
    inputs = rows[:, :model_dim]
    gradients = (rows[:, model_dim:].astype(jnp.float32) * row_gates[:, None]).astype(jnp.bfloat16)
    later_weights = (push_weights + jnp.roll(push_weights, 1)) / 2.0
    last_weights = (later_weights + jnp.roll(later_weights, 2)) / 2.0
    factor = (0.5 / last_weights + 0.5 / jnp.roll(last_weights, -2)) / node_count

    def at(values, index):
        return lax.dynamic_index_in_dim(values, index, keepdims=False)

    scalars = jnp.stack(
        [at(push_weights, node), at(later_weights, node), at(factor, node), at(factor, node ^ 1)]
    )
    return both_rounds(scalars, numerators[0, 0], inputs, gradients, node_count)[None]


def solution(mesh):
    placed = (
        P("node", "expert", None, None),
        P(),
        P("node", "expert", None),
        P("node", "expert", None),
        P("node", "expert", None),
        P("node", "expert", None),
    )
    return jax.shard_map(
        local, mesh=mesh, in_specs=placed, out_specs=P("expert", "node", None), check_vma=False
    )
```
